32 devices in a mesh: ga: 8 (over z, x), band: 4 (over y, core).
Axes of the slice: x: 2, y: 2, z: 4, core: 2. Of those that a mesh axis runs over, the one named last changes fastest.
Arguments:
- coeffs: bfloat16 [2, 512, 40960], P(None, ('ga', 'band')), may hold values from -6 to 6
- projectors: bfloat16 [1280, 2, 40960], P(None, None, 'ga'), may hold values from -0.01953125 to 0.01953125
- block_coupling: float32 [1280, 18], replicated, may hold values from -12 to 12
- atom_counts: int32 [160], replicated, may hold values from 4 to 18, as said below
- wave_counts: int32 [8], P('ga'), may hold values from 3840 to 5120
Outputs:
- applied: bfloat16 [2, 512, 40960], P(None, ('ga', 'band'))
- band_energy: float32 [512], P(('ga', 'band'))
- total_energy: float32 [], replicated
The draws below stay inside these ranges and needn't reach their ends.
Inputs may be any that keep to these rules, and one draw needn't show every extreme that they name: `atom_counts`: each atom has 4, 8 or 18 projectors, the counts sum to 1280 and the largest is 18.
All inputs are finite; a program needn't handle non-finite values.
Results may differ from the reference program's by a relative error of at most 0.013.
Values may be sent and summed in bfloat16 or wider, within the bound.
A program may use at most 128 MiB of HBM per device.

```python
import math
import jax
import jax.numpy as jnp
from jax import lax

NG = 40960
ATOMS = 160
MOST = 18
G_DEV = 5120
NB = 512
NP = 1280
N_GA = 8


def draw_atom_counts(key, part):
    group_pattern = jnp.array([18, 18, 4, 4, 4, 4, 4], jnp.int32)
    heavy_groups = ATOMS // 8
    atom_ids = lax.iota(jnp.int32, ATOMS)
    species = jnp.where(atom_ids < 7 * heavy_groups, group_pattern[atom_ids % 7], 8).astype(jnp.int32)
    return jax.random.permutation(jax.random.fold_in(key, 31), species).astype(jnp.int32)


def with_ends(entries, key, smallest, largest):
    spot = [jax.random.randint(jax.random.fold_in(key, axis), (), 0, length) for axis, length in enumerate(entries.shape)]
    widest = entries.shape.index(max(entries.shape))
    next_to = spot[:widest] + [(spot[widest] + 1) % entries.shape[widest]] + spot[widest + 1:]
    return entries.at[tuple(spot)].set(smallest).at[tuple(next_to)].set(largest)


def level_of(stream_key, extent, cuts, smallest, largest):
    loudness = 1.0
    for axis_at, shards_of in cuts:
        steps = jax.random.uniform(jax.random.fold_in(jax.random.fold_in(stream_key, 6), axis_at), (shards_of,), jnp.float32, smallest / len(cuts), largest / len(cuts))
        loudness = loudness * jnp.repeat(jnp.exp(steps), extent[axis_at] // shards_of).reshape((-1,) + (1,) * (len(extent) - 1 - axis_at))
    return loudness


def noise(own_key, extent, spread, most, pieces=(), kind=jnp.bfloat16):
    gain = level_of(own_key, extent, pieces, -0.22, 0.18) if pieces else 1.0
    values = jax.random.normal(own_key, extent, jnp.float32) * spread * gain
    return jnp.minimum(jnp.maximum(values, -most), most).astype(kind)


def setup_inputs(seed: int = 0) -> dict:
    streams_of = jax.random.split(jax.random.key(seed), 6)
    return {
        "coeffs": noise(streams_of[0], (2, NB, NG), 1.0, 6.0, ((1, 32),)),
        "projectors": noise(streams_of[1], (NP, 2, NG), (2 * NG) ** -0.5, 0.01953125, ((2, 8),)),
        "block_coupling": noise(streams_of[2], (NP, MOST), 2.0, 12.0, (), jnp.float32),
        "atom_counts": draw_atom_counts(jax.random.fold_in(streams_of[5], 71), 0),
        "wave_counts": with_ends(jax.random.randint(streams_of[4], (N_GA,), G_DEV * 3 // 4, G_DEV + 1), jax.random.fold_in(streams_of[4], 1), G_DEV * 3 // 4, G_DEV).astype(jnp.int32),
    }


def block_tables(atom_counts, row_ids):
    atom_ends = jnp.cumsum(atom_counts).astype(jnp.int32)
    atom_starts = (atom_ends - atom_counts).astype(jnp.int32)
    inside = (atom_starts[None, :] <= row_ids[:, None]) & (atom_ends[None, :] > row_ids[:, None])
    block_first = lax.optimization_barrier(jnp.sum(jnp.where(inside, atom_starts[None, :], 0), axis=1)).astype(jnp.int32)
    block_length = lax.optimization_barrier(jnp.sum(jnp.where(inside, atom_counts[None, :], 0), axis=1)).astype(jnp.int32)
    return (block_first, block_length)

def couple_rows(values, block_first, block_length, coupling_rows, row_base):
    last_row = values.shape[0] - 1
    summed = jnp.zeros((coupling_rows.shape[0], values.shape[1]), jnp.float32)
    for offset in range(coupling_rows.shape[1]):
        source = jnp.clip(block_first + offset - row_base, 0, last_row).astype(jnp.int32)
        column = coupling_rows[:, offset]
        weight = jnp.where(offset < block_length, column, jnp.zeros_like(column))
        summed = summed + weight[:, None] * jnp.take(values, source, axis=0)
    return summed

def reference(coeffs, projectors, block_coupling, atom_counts, wave_counts):
    slot_ids = lax.iota(jnp.int32, NG)
    in_sphere = (slot_ids % G_DEV < wave_counts[slot_ids // G_DEV]).astype(jnp.float32)
    masked = coeffs * in_sphere.astype(coeffs.dtype)
    real_part = masked[0]
    imag_part = masked[1]
    stacked = jnp.concatenate([jnp.concatenate([real_part, imag_part], 1), jnp.concatenate([imag_part, -real_part], 1)], 0)
    flat_beta = projectors.reshape(NP, 2 * NG)
    projections = lax.dot_general(flat_beta, stacked, (((1,), (1,)), ((), ())), preferred_element_type=jnp.float32)
    block_first, block_length = block_tables(atom_counts, lax.iota(jnp.int32, NP))
    coupled = couple_rows(projections, block_first, block_length, block_coupling, 0)
    energy_terms = lax.optimization_barrier(jnp.sum(projections * coupled, axis=0))
    band_energy = (energy_terms[:NB] + energy_terms[NB:]) / NP
    total_energy = jnp.sum(band_energy) / math.sqrt(NB)
    products = lax.dot_general(coupled.astype(jnp.bfloat16), flat_beta, (((0,), (0,)), ((), ())), preferred_element_type=jnp.float32)
    real_out = products[:NB, :NG] - products[NB:, NG:]
    imag_out = products[:NB, NG:] + products[NB:, :NG]
    applied = (jnp.stack([real_out, imag_out]) * in_sphere).astype(jnp.bfloat16)
    return (applied, band_energy, total_energy)
```

```python
import functools
import math

import jax
import jax.numpy as jnp
from jax import lax
from jax.experimental import pallas as pl
from jax.experimental.pallas import tpu as pltpu
from jax.sharding import PartitionSpec as P

MESH = pl.DeviceIdType.MESH
PIECES = 4
STAGE = 128
ROWS = 512


def divisor(total, most, unit):
    size = min(most, total)
    while total % size or size % unit:
        size -= unit
    return size


def diagonals(block_coupling, atom_counts):
    rows, most = block_coupling.shape
    atoms = atom_counts.shape[0]
    earlier = lax.iota(jnp.int32, atoms)[None, :] < lax.iota(jnp.int32, atoms)[:, None]
    starts = jnp.sum(jnp.where(earlier, atom_counts[None, :], 0), axis=1)
    ids = lax.iota(jnp.int32, rows)
    inside = (starts[:, None] <= ids[None, :]) & ((starts + atom_counts)[:, None] > ids[None, :])
    first = jnp.sum(jnp.where(inside, starts[:, None], 0), axis=0)
    length = jnp.sum(jnp.where(inside, atom_counts[:, None], 0), axis=0)
    place = ids - first
    shift = lax.broadcasted_iota(jnp.int32, (2 * most - 1, rows), 0) - (most - 1)
    column = shift + place[None, :]
    fits = column < length[None, :]
    table = jnp.zeros((2 * most - 1, rows), jnp.float32)
    for k in range(most):
        table = jnp.where(fits & (column == k), block_coupling[:, k][None, :], table)
    return jnp.repeat(table, 2, axis=1)


def swap_pairs(values, even_sign, odd_sign):
    lanes = values.shape[-1]
    even = lax.rem(lax.broadcasted_iota(jnp.int32, values.shape, values.ndim - 1), 2) == 0
    up = pltpu.roll(values, lanes - 1, values.ndim - 1)
    down = pltpu.roll(values, 1, values.ndim - 1)
    return jnp.where(even, even_sign * up, odd_sign * down)


def kernel(
    n, nb, counts, coeffs, beta, table, out, energy, total,
    stage, held, xbuf, xt, acc, usend, urecv, dsend, drecv, dfull, obuf,
    esend, erecv, gsend, grecv,
    stage_sem, own_sem, xs, xr, us, ur, ds_, dr, os_, or_, es, er, gs, gr, oown,
):
    me = lax.axis_index("ga")
    mb = lax.axis_index("band")
    own = coeffs.shape[1]
    slots = beta.shape[2]
    rows = held.shape[0]
    bands = n * own
    piece = slots // PIECES
    order = sorted(range(1, n), key=lambda t: -min(t, n - t))
    peers = [lax.rem(me + t, n) for t in order]
    mates = [lax.rem(mb + t, nb) for t in range(1, nb)]

    def stage_copy(i, slot):
        return pltpu.make_async_copy(
            beta.at[pl.ds(i * STAGE, STAGE)], stage.at[slot], stage_sem.at[slot]
        )

    def own_x(c):
        return pltpu.make_async_copy(
            coeffs.at[:, :, pl.ds(pl.multiple_of(me * slots + c * piece, 128), piece)],
            xbuf.at[c, :, me],
            own_sem.at[c],
        )

    def x_copy(c, j, source):
        return pltpu.make_async_remote_copy(
            src_ref=coeffs.at[:, :, pl.ds(pl.multiple_of(j * slots + c * piece, 128), piece)],
            dst_ref=xbuf.at[c, :, source],
            send_sem=xs.at[c, j],
            recv_sem=xr.at[c, source],
            device_id={"ga": j},
            device_id_type=MESH,
        )

    def u_copy(j, source):
        return pltpu.make_async_remote_copy(
            src_ref=usend.at[j], dst_ref=urecv.at[source],
            send_sem=us.at[j], recv_sem=ur.at[source],
            device_id={"ga": j}, device_id_type=MESH,
        )

    def d_copy(j, source):
        return pltpu.make_async_remote_copy(
            src_ref=dsend, dst_ref=drecv.at[source],
            send_sem=ds_.at[j], recv_sem=dr.at[source],
            device_id={"ga": j}, device_id_type=MESH,
        )

    def e_copy(j, source):
        return pltpu.make_async_remote_copy(
            src_ref=esend, dst_ref=erecv.at[source],
            send_sem=es.at[j], recv_sem=er.at[source],
            device_id={"ga": j}, device_id_type=MESH,
        )

    def g_copy(j, source):
        return pltpu.make_async_remote_copy(
            src_ref=gsend, dst_ref=grecv.at[source],
            send_sem=gs.at[j], recv_sem=gr.at[source],
            device_id={"band": j}, device_id_type=MESH,
        )

    def o_copy(c, j, source):
        return pltpu.make_async_remote_copy(
            src_ref=obuf.at[c, :, j],
            dst_ref=out.at[:, :, pl.ds(pl.multiple_of(source * slots + c * piece, 128), piece)],
            send_sem=os_.at[c, j],
            recv_sem=or_.at[c, source],
            device_id={"ga": j},
            device_id_type=MESH,
        )

    def own_o(c):
        return pltpu.make_async_copy(
            obuf.at[c, :, me],
            out.at[:, :, pl.ds(pl.multiple_of(me * slots + c * piece, 128), piece)],
            oown.at[c],
        )

    stage_copy(0, 0).start()
    barrier = pltpu.get_barrier_semaphore()
    for j in peers:
        pl.semaphore_signal(barrier, inc=1, device_id={"ga": j}, device_id_type=MESH)
    for j in mates:
        pl.semaphore_signal(barrier, inc=1, device_id={"band": j}, device_id_type=MESH)
    pl.semaphore_wait(barrier, n - 1 + nb - 1)

    for c in range(PIECES):
        for j in peers:
            x_copy(c, j, me).start()
    for c in range(PIECES):
        own_x(c).start()

    blocks = beta.shape[0] // STAGE
    width = divisor(slots, 512, 128)

    def lay(i, carry):
        slot = lax.rem(i, 2)

        @pl.when(i + 1 < blocks)
        def _():
            stage_copy(i + 1, 1 - slot).start()

        stage_copy(i, slot).wait()

        def cols(w, carry):
            at = pl.ds(pl.multiple_of(w * width, 128), width)
            held[pl.ds(pl.multiple_of(i * 2 * STAGE, 2 * STAGE), 2 * STAGE), at] = stage[
                slot, :, :, at
            ].reshape(2 * STAGE, width)
            return carry

        return lax.fori_loop(0, slots // width, cols, carry)

    lax.fori_loop(0, blocks, lay, 0)

    count = counts[0]
    for c in range(PIECES):
        own_x(c).wait()
        for j in peers:
            x_copy(c, j, j).wait_recv()
        slot_ids = c * piece + lax.broadcasted_iota(jnp.int32, (2 * bands, piece), 1)
        block = xbuf[c].reshape(2 * bands, piece).astype(jnp.float32)
        xt[...] = jnp.where(slot_ids < count, block, 0.0).T.astype(jnp.bfloat16)

        def product(r, carry, c=c):
            at = pl.ds(pl.multiple_of(r * ROWS, ROWS), ROWS)
            term = jnp.dot(
                held[at, c * piece : (c + 1) * piece], xt[...], preferred_element_type=jnp.float32
            )
            if c > 0:
                term = term + acc[at, :]
            if c < PIECES - 1:
                acc[at, :] = term
            else:
                turned = term.T
                united = turned[:bands] + swap_pairs(turned[bands:], 1.0, -1.0)
                usend[:, :, at] = united.astype(jnp.bfloat16).reshape(n, own, ROWS)
            return carry

        lax.fori_loop(0, rows // ROWS, product, 0)

    for j in peers:
        u_copy(j, me).start()
    summed = usend[me].astype(jnp.float32)
    for j in peers:
        u_copy(j, j).wait_recv()
        summed = summed + urecv[j].astype(jnp.float32)
    most = (table.shape[0] + 1) // 2
    coupled = summed * table[most - 1 : most, :]
    for d in range(1 - most, most):
        if d:
            moved = pltpu.roll(summed, (-2 * d) % rows, 1)
            coupled = coupled + moved * table[most - 1 + d : most + d, :]
    dsend[...] = coupled.astype(jnp.bfloat16)
    for j in peers:
        d_copy(j, me).start()
    drecv[me] = coupled.astype(jnp.bfloat16)
    band_energy = jnp.sum(summed * coupled, axis=1, keepdims=True) / beta.shape[0]
    energy[...] = jnp.broadcast_to(band_energy, energy.shape)
    esend[...] = jnp.broadcast_to(jnp.sum(band_energy, axis=0, keepdims=True), esend.shape)
    for j in peers:
        e_copy(j, me).start()

    for j in peers:
        d_copy(j, j).wait_recv()
    real = drecv[...].reshape(bands, rows).astype(jnp.float32)
    dfull[:bands, :] = real.astype(jnp.bfloat16)
    dfull[bands:, :] = swap_pairs(real, -1.0, 1.0).astype(jnp.bfloat16)

    step = divisor(piece, 256, 128)
    for c in range(PIECES):

        def apply(w, carry, c=c):
            lanes = pl.ds(pl.multiple_of(w * step, 128), step)
            slab = pl.ds(pl.multiple_of(c * piece + w * step, 128), step)
            result = jnp.dot(dfull[...], held[:, slab], preferred_element_type=jnp.float32)
            ids = c * piece + w * step + lax.broadcasted_iota(jnp.int32, result.shape, 1)
            result = jnp.where(ids < count, result, 0.0).astype(jnp.bfloat16)
            obuf[c, :, :, :, lanes] = result.reshape(2, n, own, step)
            return carry

        lax.fori_loop(0, piece // step, apply, 0)
        for j in peers:
            o_copy(c, j, me).start()
        own_o(c).start()

    group = esend[...]
    for j in peers:
        e_copy(j, j).wait_recv()
        group = group + erecv[j]
    gsend[...] = group
    for j in mates:
        g_copy(j, mb).start()
    whole = group
    for j in mates:
        g_copy(j, j).wait_recv()
        whole = whole + grecv[j]
    total[...] = whole / math.sqrt(n * nb * own)

    for c in range(PIECES):
        for j in peers:
            x_copy(c, j, me).wait_send()
            o_copy(c, j, me).wait_send()
            o_copy(c, j, j).wait_recv()
        own_o(c).wait()
    for j in peers:
        u_copy(j, me).wait_send()
        d_copy(j, me).wait_send()
        e_copy(j, me).wait_send()
    for j in mates:
        g_copy(j, mb).wait_send()


def shards(n, nb, coeffs, projectors, block_coupling, atom_counts, wave_counts):
    own = coeffs.shape[1]
    count, _, slots = projectors.shape
    rows = 2 * count
    bands = n * own
    piece = slots // PIECES
    low, full = jnp.bfloat16, jnp.float32
    dma = pltpu.SemaphoreType.DMA
    table = diagonals(block_coupling, atom_counts)
    flops = 4 * rows * slots * 2 * bands
    out, energy, total = pl.pallas_call(
        functools.partial(kernel, n, nb),
        out_shape=(
            jax.ShapeDtypeStruct(coeffs.shape, low),
            jax.ShapeDtypeStruct((own, 128), full),
            jax.ShapeDtypeStruct((8, 128), full),
        ),
        in_specs=[
            pl.BlockSpec(memory_space=pltpu.SMEM),
            pl.BlockSpec(memory_space=pl.ANY),
            pl.BlockSpec(memory_space=pl.ANY),
            pl.BlockSpec(memory_space=pltpu.VMEM),
        ],
        out_specs=(
            pl.BlockSpec(memory_space=pl.ANY),
            pl.BlockSpec(memory_space=pltpu.VMEM),
            pl.BlockSpec(memory_space=pltpu.VMEM),
        ),
        scratch_shapes=[
            pltpu.VMEM((2, STAGE, 2, slots), low),
            pltpu.VMEM((rows, slots), low),
            pltpu.VMEM((PIECES, 2, n, own, piece), low),
            pltpu.VMEM((piece, 2 * bands), low),
            pltpu.VMEM((rows, 2 * bands), full),
            pltpu.VMEM((n, own, rows), low),
            pltpu.VMEM((n, own, rows), low),
            pltpu.VMEM((own, rows), low),
            pltpu.VMEM((n, own, rows), low),
            pltpu.VMEM((2 * bands, rows), low),
            pltpu.VMEM((PIECES, 2, n, own, piece), low),
            pltpu.VMEM((8, 128), full),
            pltpu.VMEM((n, 8, 128), full),
            pltpu.VMEM((8, 128), full),
            pltpu.VMEM((nb, 8, 128), full),
            dma((2,)),
            dma((PIECES,)),
            dma((PIECES, n)),
            dma((PIECES, n)),
            dma((n,)),
            dma((n,)),
            dma((n,)),
            dma((n,)),
            dma((PIECES, n)),
            dma((PIECES, n)),
            dma((n,)),
            dma((n,)),
            dma((nb,)),
            dma((nb,)),
            dma((PIECES,)),
        ],
        compiler_params=pltpu.CompilerParams(
            collective_id=0, has_side_effects=True, vmem_limit_bytes=62 * 2**20
        ),
        cost_estimate=pl.CostEstimate(
            flops=flops, bytes_accessed=2 * rows * slots, transcendentals=0
        ),
    )(wave_counts, coeffs, projectors, table)
    return (out, energy[:, 0], total[0, 0])


def solution(mesh):
    placed = (P(None, ("ga", "band"), None), P(None, None, "ga"), P(), P(), P("ga"))
    return jax.shard_map(
        functools.partial(shards, mesh.shape["ga"], mesh.shape["band"]),
        mesh=mesh,
        in_specs=placed,
        out_specs=(P(None, ("ga", "band"), None), P(("ga", "band")), P()),
        check_vma=False,
    )
```

```python
import functools
import math

import jax
import jax.numpy as jnp
from jax import lax
from jax.experimental import pallas as pl
from jax.experimental.pallas import tpu as pltpu
from jax.sharding import PartitionSpec as P

MESH = pl.DeviceIdType.MESH
HALVES = 2
PIECES = 4
STAGE = 128
ROWS = 512


def divisor(total, most, unit):
    size = min(most, total)
    while total % size or size % unit:
        size -= unit
    return size


def diagonals(counts, coupling):
    atoms = counts.shape[1]
    most, rows = coupling.shape
    counts = counts.astype(jnp.float32)
    square = (atoms, atoms)
    across = lax.broadcasted_iota(jnp.int32, square, 1)
    down = lax.broadcasted_iota(jnp.int32, square, 0)
    starts = jnp.sum(jnp.where(across < down, counts, 0.0), axis=1, keepdims=True)
    sizes = jnp.sum(jnp.where(across == down, counts, 0.0), axis=1, keepdims=True)
    ids = lax.broadcasted_iota(jnp.int32, (atoms, rows), 1).astype(jnp.float32)
    inside = (starts <= ids) & (ids < starts + sizes)
    first = jnp.sum(jnp.where(inside, starts, 0.0), axis=0, keepdims=True)
    length = jnp.sum(jnp.where(inside, sizes, 0.0), axis=0, keepdims=True)
    shape = (2 * most - 1, rows)
    shift = lax.broadcasted_iota(jnp.int32, shape, 0) - (most - 1)
    place = lax.broadcasted_iota(jnp.int32, shape, 1) - first.astype(jnp.int32)
    column = shift + place
    fits = column < length.astype(jnp.int32)
    table = jnp.zeros(shape, jnp.float32)
    for k in range(most):
        table = jnp.where(fits & (column == k), coupling[k : k + 1, :], table)
    unit = divisor(rows, 128, 128)
    wide = lax.broadcasted_iota(jnp.int32, (unit, 2 * unit), 1)
    source = lax.broadcasted_iota(jnp.int32, (unit, 2 * unit), 0)
    twice = ((wide == 2 * source) | (wide == 2 * source + 1)).astype(jnp.float32)
    return [
        jnp.dot(
            table[:, at : at + unit],
            twice,
            precision=lax.Precision.HIGHEST,
            preferred_element_type=jnp.float32,
        )
        for at in range(0, rows, unit)
    ]


def swap_pairs(values, even_sign, odd_sign):
    lanes = values.shape[-1]
    even = lax.rem(lax.broadcasted_iota(jnp.int32, values.shape, values.ndim - 1), 2) == 0
    up = pltpu.roll(values, lanes - 1, values.ndim - 1)
    down = pltpu.roll(values, 1, values.ndim - 1)
    return jnp.where(even, even_sign * up, odd_sign * down)


def kernel(
    n, nb, counts, coeffs, beta, coupling, atoms, out, energy, total,
    stage, held, xbuf, xt, acc, table, usend, urecv, usum, csend, crecv, dsend, drecv, dfull,
    obuf, esend, erecv, gsend, grecv,
    stage_sem, own_sem, xs, xr, us, ur, cs, cr, ds_, fs, bs, dr, os_, or_, es, er, gs, gr, oown,
):
    me = lax.axis_index("ga")
    mb = lax.axis_index("band")
    slots = beta.shape[2]
    rows = held.shape[0]
    own = coeffs.shape[1]
    part = own // HALVES
    bands = n * part
    piece = slots // PIECES
    near = n // 2
    side, spot = me // near, lax.rem(me, near)
    other = lax.rem(me + near, n)
    order = sorted(range(1, n), key=lambda t: -min(t, n - t))
    peers = [lax.rem(me + t, n) for t in order]
    mates = [lax.rem(mb + t, nb) for t in range(1, nb)]
    spots = [lax.rem(spot + t, near) for t in range(1, near)]

    def remote(src, dst, send, recv, j, axis="ga"):
        return pltpu.make_async_remote_copy(
            src_ref=src, dst_ref=dst, send_sem=send, recv_sem=recv,
            device_id={axis: j}, device_id_type=MESH,
        )

    def stage_copy(i, slot):
        return pltpu.make_async_copy(
            beta.at[pl.ds(i * STAGE, STAGE)], stage.at[slot], stage_sem.at[slot]
        )

    def x_part(h, c, j):
        at = pl.ds(pl.multiple_of(j * slots + c * piece, 128), piece)
        return coeffs.at[:, h * part : (h + 1) * part, at]

    def o_part(h, c, j):
        at = pl.ds(pl.multiple_of(j * slots + c * piece, 128), piece)
        return out.at[:, h * part : (h + 1) * part, at]

    def own_x(h, c):
        return pltpu.make_async_copy(x_part(h, c, me), xbuf.at[h, c, :, me], own_sem.at[h, c])

    def x_copy(h, c, j, source):
        return remote(
            x_part(h, c, j), xbuf.at[h, c, :, source], xs.at[h, c, j], xr.at[h, c, source], j
        )

    def own_o(h, c):
        return pltpu.make_async_copy(obuf.at[h, c, :, me], o_part(h, c, me), oown.at[h, c])

    def o_copy(h, c, j, source):
        return remote(
            obuf.at[h, c, :, j], o_part(h, c, source), os_.at[h, c, j], or_.at[h, c, source], j
        )

    def u_copy(h, at, source):
        return remote(
            usend.at[h, :, at], urecv.at[h, source], us.at[h, at], ur.at[h, source],
            side * near + at,
        )

    def c_copy(h):
        return remote(csend.at[h], crecv.at[h], cs.at[h], cr.at[h], other)

    def d_copy(h, at, source):
        return remote(
            dsend.at[h], drecv.at[h, side * near + source], ds_.at[h, at],
            dr.at[h, side * near + source], side * near + at,
        )

    def b_copy(h, source):
        return remote(dsend.at[h], drecv.at[h, source], bs.at[h], dr.at[h, source], other)

    def f_copy(h, at, source):
        block = drecv.at[h, (1 - side) * near + source]
        return remote(
            block, block, fs.at[h, at], dr.at[h, (1 - side) * near + source], side * near + at
        )

    def e_copy(j, source):
        return remote(esend, erecv.at[source], es.at[j], er.at[source], j)

    def g_copy(j, source):
        return remote(gsend, grecv.at[source], gs.at[j], gr.at[source], j, "band")

    def send_x(h, c):
        for j in peers:
            x_copy(h, c, j, me).start()

    count = counts[0]

    def first_product(h, c):
        own_x(h, c).wait()
        for j in peers:
            x_copy(h, c, j, j).wait_recv()
        slot_ids = c * piece + lax.broadcasted_iota(jnp.int32, (2 * bands, piece), 1)
        block = xbuf[h, c].astype(jnp.float32).reshape(2 * bands, piece)
        xt[...] = jnp.where(slot_ids < count, block, 0.0).T.astype(jnp.bfloat16)

        def product(r, carry):
            at = pl.ds(pl.multiple_of(r * ROWS, ROWS), ROWS)
            term = jnp.dot(
                held[at, c * piece : (c + 1) * piece], xt[...], preferred_element_type=jnp.float32
            )
            if c > 0:
                term = term + acc[at, :]
            if c < PIECES - 1:
                acc[at, :] = term
            else:
                turned = term.T
                united = turned[:bands] + swap_pairs(turned[bands:], 1.0, -1.0)
                united = united.reshape(2, near, part, ROWS)
                usend[h, :, :, :, at] = united.astype(jnp.bfloat16)
            return carry

        lax.fori_loop(0, rows // ROWS, product, 0)

    def send_sums(h):
        for at in spots:
            u_copy(h, at, spot).start()

    def half_sums(h):
        same = usend[h, side, spot].astype(jnp.float32)
        away = usend[h, 1 - side, spot].astype(jnp.float32)
        for at in spots:
            u_copy(h, at, at).wait_recv()
            same = same + urecv[h, at, side].astype(jnp.float32)
            away = away + urecv[h, at, 1 - side].astype(jnp.float32)
        csend[h] = away.astype(jnp.bfloat16)
        c_copy(h).start()
        usum[h] = same

    def couple(h):
        c_copy(h).wait_recv()
        summed = usum[h] + crecv[h].astype(jnp.float32)
        most = (table.shape[0] + 1) // 2
        coupled = summed * table[most - 1 : most, :]
        for d in range(1 - most, most):
            if d:
                moved = pltpu.roll(summed, (-2 * d) % rows, 1)
                coupled = coupled + moved * table[most - 1 + d : most + d, :]
        low = coupled.astype(jnp.bfloat16)
        dsend[h] = low
        b_copy(h, me).start()
        for at in spots:
            d_copy(h, at, spot).start()
        drecv[h, me] = low
        bands_now = jnp.sum(summed * coupled, axis=1, keepdims=True) / beta.shape[0]
        lanes = lax.broadcasted_iota(jnp.int32, (part, own), 1)
        line = lax.broadcasted_iota(jnp.int32, (part, own), 0) + h * part
        row = jnp.sum(jnp.where(lanes == line, bands_now, 0.0), axis=0, keepdims=True)
        sofar = jnp.broadcast_to(jnp.sum(bands_now, axis=0, keepdims=True), esend.shape)
        if h == 0:
            energy[...] = row
            gsend[...] = sofar
        else:
            energy[...] = energy[...] + row
            esend[...] = gsend[...] + sofar
            for j in peers:
                e_copy(j, me).start()

    def pass_on(h):
        b_copy(h, other).wait_recv()
        for at in spots:
            f_copy(h, at, spot).start()

    def gather(h):
        for at in spots:
            d_copy(h, at, at).wait_recv()
            f_copy(h, at, at).wait_recv()
        real = drecv[h].astype(jnp.float32).reshape(bands, rows)
        dfull[:bands, :] = real.astype(jnp.bfloat16)
        dfull[bands:, :] = swap_pairs(real, -1.0, 1.0).astype(jnp.bfloat16)

    step = divisor(piece, 256, 128)

    def second_product(h, c):
        def apply(w, carry):
            lanes = pl.ds(pl.multiple_of(w * step, 128), step)
            slab = pl.ds(pl.multiple_of(c * piece + w * step, 128), step)
            result = jnp.dot(dfull[...], held[:, slab], preferred_element_type=jnp.float32)
            ids = c * piece + w * step + lax.broadcasted_iota(jnp.int32, result.shape, 1)
            result = jnp.where(ids < count, result, 0.0).reshape(2, n, part, step)
            obuf[h, c, :, :, :, lanes] = result.astype(jnp.bfloat16)
            return carry

        lax.fori_loop(0, piece // step, apply, 0)
        for j in peers:
            o_copy(h, c, j, me).start()
        own_o(h, c).start()

    stage_copy(0, 0).start()
    barrier = pltpu.get_barrier_semaphore()
    for j in peers:
        pl.semaphore_signal(barrier, inc=1, device_id={"ga": j}, device_id_type=MESH)
    for j in mates:
        pl.semaphore_signal(barrier, inc=1, device_id={"band": j}, device_id_type=MESH)
    pl.semaphore_wait(barrier, n - 1 + nb - 1)

    for c in range(PIECES):
        send_x(0, c)
    early = PIECES // 2
    for c in range(early):
        send_x(1, c)
    for h in range(HALVES):
        for c in range(PIECES):
            own_x(h, c).start()

    blocks = beta.shape[0] // STAGE
    width = divisor(slots, 512, 128)

    def lay(i, carry):
        slot = lax.rem(i, 2)

        @pl.when(i + 1 < blocks)
        def _():
            stage_copy(i + 1, 1 - slot).start()

        stage_copy(i, slot).wait()

        def cols(w, carry):
            at = pl.ds(pl.multiple_of(w * width, 128), width)
            held[pl.ds(pl.multiple_of(i * 2 * STAGE, 2 * STAGE), 2 * STAGE), at] = stage[
                slot, :, :, at
            ].reshape(2 * STAGE, width)
            return carry

        return lax.fori_loop(0, slots // width, cols, carry)

    lax.fori_loop(0, blocks, lay, 0)
    strips = diagonals(atoms[...], coupling[...])
    wide = rows // len(strips)
    for i, strip in enumerate(strips):
        table[:, i * wide : (i + 1) * wide] = strip

    for c in range(PIECES):
        first_product(0, c)
    send_sums(0)
    for c in range(early, PIECES - 1):
        send_x(1, c)
    first_product(1, 0)
    half_sums(0)
    send_x(1, PIECES - 1)
    first_product(1, 1)
    couple(0)
    for c in range(2, PIECES - 1):
        first_product(1, c)
    pass_on(0)
    first_product(1, PIECES - 1)
    send_sums(1)
    gather(0)
    second_product(0, 0)
    half_sums(1)
    second_product(0, 1)
    couple(1)
    for c in range(2, PIECES - 1):
        second_product(0, c)
    pass_on(1)
    second_product(0, PIECES - 1)
    gather(1)
    for c in range(PIECES):
        second_product(1, c)

    for j in peers:
        e_copy(j, me).wait_send()
    group = esend[...]
    for j in peers:
        e_copy(j, j).wait_recv()
        group = group + erecv[j]
    gsend[...] = group
    for j in mates:
        g_copy(j, mb).start()
    whole = group
    for j in mates:
        g_copy(j, j).wait_recv()
        whole = whole + grecv[j]
    total[...] = whole[:1, :1] / math.sqrt(n * nb * own)

    for j in mates:
        g_copy(j, mb).wait_send()
    for h in range(HALVES):
        for c in range(PIECES):
            for j in peers:
                x_copy(h, c, j, me).wait_send()
                o_copy(h, c, j, me).wait_send()
                o_copy(h, c, j, j).wait_recv()
            own_o(h, c).wait()
        for at in spots:
            u_copy(h, at, spot).wait_send()
            d_copy(h, at, spot).wait_send()
            f_copy(h, at, spot).wait_send()
        c_copy(h).wait_send()
        b_copy(h, me).wait_send()


def shards(n, nb, coeffs, projectors, block_coupling, atom_counts, wave_counts):
    own = coeffs.shape[1]
    count, _, slots = projectors.shape
    most = block_coupling.shape[1]
    rows = 2 * count
    part = own // HALVES
    bands = n * part
    near = n // 2
    piece = slots // PIECES
    low, full = jnp.bfloat16, jnp.float32
    dma = pltpu.SemaphoreType.DMA
    out, energy, total = pl.pallas_call(
        functools.partial(kernel, n, nb),
        out_shape=(
            jax.ShapeDtypeStruct(coeffs.shape, low),
            jax.ShapeDtypeStruct((1, own), full),
            jax.ShapeDtypeStruct((1, 1), full),
        ),
        in_specs=[
            pl.BlockSpec(memory_space=pltpu.SMEM),
            pl.BlockSpec(memory_space=pl.ANY),
            pl.BlockSpec(memory_space=pl.ANY),
            pl.BlockSpec(memory_space=pltpu.VMEM),
            pl.BlockSpec(memory_space=pltpu.VMEM),
        ],
        out_specs=(
            pl.BlockSpec(memory_space=pl.ANY),
            pl.BlockSpec(memory_space=pltpu.VMEM),
            pl.BlockSpec(memory_space=pltpu.VMEM),
        ),
        scratch_shapes=[
            pltpu.VMEM((2, STAGE, 2, slots), low),
            pltpu.VMEM((rows, slots), low),
            pltpu.VMEM((HALVES, PIECES, 2, n, part, piece), low),
            pltpu.VMEM((piece, 2 * bands), low),
            pltpu.VMEM((rows, 2 * bands), full),
            pltpu.VMEM((2 * most - 1, rows), full),
            pltpu.VMEM((HALVES, 2, near, part, rows), low),
            pltpu.VMEM((HALVES, near, 2, part, rows), low),
            pltpu.VMEM((HALVES, part, rows), full),
            pltpu.VMEM((HALVES, part, rows), low),
            pltpu.VMEM((HALVES, part, rows), low),
            pltpu.VMEM((HALVES, part, rows), low),
            pltpu.VMEM((HALVES, n, part, rows), low),
            pltpu.VMEM((2 * bands, rows), low),
            pltpu.VMEM((HALVES, PIECES, 2, n, part, piece), low),
            pltpu.VMEM((8, 128), full),
            pltpu.VMEM((n, 8, 128), full),
            pltpu.VMEM((8, 128), full),
            pltpu.VMEM((nb, 8, 128), full),
            dma((2,)),
            dma((HALVES, PIECES)),
            dma((HALVES, PIECES, n)),
            dma((HALVES, PIECES, n)),
            dma((HALVES, near)),
            dma((HALVES, near)),
            dma((HALVES,)),
            dma((HALVES,)),
            dma((HALVES, near)),
            dma((HALVES, near)),
            dma((HALVES,)),
            dma((HALVES, n)),
            dma((HALVES, PIECES, n)),
            dma((HALVES, PIECES, n)),
            dma((n,)),
            dma((n,)),
            dma((nb,)),
            dma((nb,)),
            dma((HALVES, PIECES)),
        ],
        compiler_params=pltpu.CompilerParams(
            collective_id=0, has_side_effects=True, vmem_limit_bytes=62 * 2**20
        ),
        cost_estimate=pl.CostEstimate(
            flops=8 * rows * slots * n * own, bytes_accessed=2 * rows * slots, transcendentals=0
        ),
    )(wave_counts, coeffs, projectors, block_coupling.T, atom_counts.reshape(1, -1))
    return (out, energy.reshape(own), total.reshape(()))


def solution(mesh):
    placed = (P(None, ("ga", "band"), None), P(None, None, "ga"), P(), P(), P("ga"))
    return jax.shard_map(
        functools.partial(shards, mesh.shape["ga"], mesh.shape["band"]),
        mesh=mesh,
        in_specs=placed,
        out_specs=(P(None, ("ga", "band"), None), P(("ga", "band")), P()),
        check_vma=False,
    )
```

```python
import functools
import math

import jax
import jax.numpy as jnp
from jax import lax
from jax.experimental import pallas as pl
from jax.experimental.pallas import tpu as pltpu
from jax.sharding import PartitionSpec as P

MESH = pl.DeviceIdType.MESH
HALVES = 2
PIECES = 4
STAGE = 128
ROWS = 512


def divisor(total, most, unit):
    size = min(most, total)
    while total % size or size % unit:
        size -= unit
    return size


def diagonals(counts, coupling):
    atoms = counts.shape[1]
    most, rows = coupling.shape
    counts = counts.astype(jnp.float32)
    square = (atoms, atoms)
    across = lax.broadcasted_iota(jnp.int32, square, 1)
    down = lax.broadcasted_iota(jnp.int32, square, 0)
    starts = jnp.sum(jnp.where(across < down, counts, 0.0), axis=1, keepdims=True)
    sizes = jnp.sum(jnp.where(across == down, counts, 0.0), axis=1, keepdims=True)
    ids = lax.broadcasted_iota(jnp.int32, (atoms, rows), 1).astype(jnp.float32)
    inside = (starts <= ids) & (ids < starts + sizes)
    first = jnp.sum(jnp.where(inside, starts, 0.0), axis=0, keepdims=True)
    length = jnp.sum(jnp.where(inside, sizes, 0.0), axis=0, keepdims=True)
    shape = (2 * most - 1, rows)
    shift = lax.broadcasted_iota(jnp.int32, shape, 0) - (most - 1)
    place = lax.broadcasted_iota(jnp.int32, shape, 1) - first.astype(jnp.int32)
    column = shift + place
    fits = column < length.astype(jnp.int32)
    table = jnp.zeros(shape, jnp.float32)
    for k in range(most):
        table = jnp.where(fits & (column == k), coupling[k : k + 1, :], table)
    unit = divisor(rows, 128, 128)
    wide = lax.broadcasted_iota(jnp.int32, (unit, 2 * unit), 1)
    source = lax.broadcasted_iota(jnp.int32, (unit, 2 * unit), 0)
    twice = ((wide == 2 * source) | (wide == 2 * source + 1)).astype(jnp.float32)
    return [
        jnp.dot(
            table[:, at : at + unit],
            twice,
            precision=lax.Precision.HIGHEST,
            preferred_element_type=jnp.float32,
        )
        for at in range(0, rows, unit)
    ]


def swap_pairs(values, even_sign, odd_sign):
    lanes = values.shape[-1]
    even = lax.rem(lax.broadcasted_iota(jnp.int32, values.shape, values.ndim - 1), 2) == 0
    up = pltpu.roll(values, lanes - 1, values.ndim - 1)
    down = pltpu.roll(values, 1, values.ndim - 1)
    return jnp.where(even, even_sign * up, odd_sign * down)


def kernel(
    n, nb, counts, coeffs, beta, coupling, atoms, out, energy, total,
    stage, held, xbuf, xt, acc, table, usend, urecv, usum, csend, crecv, dsend, drecv, dfull,
    obuf, esend, erecv, gsend, grecv,
    stage_sem, own_sem, xs, xr, us, ur, cs, cr, ds_, fs, bs, dr, os_, or_, es, er, gs, gr, oown,
):
    me = lax.axis_index("ga")
    mb = lax.axis_index("band")
    slots = beta.shape[2]
    rows = held.shape[0]
    own = coeffs.shape[1]
    part = own // HALVES
    bands = n * part
    piece = slots // PIECES
    near = n // 2
    side, spot = me // near, lax.rem(me, near)
    other = lax.rem(me + near, n)
    order = sorted(range(1, n), key=lambda t: -min(t, n - t))
    peers = [lax.rem(me + t, n) for t in order]
    mates = [lax.rem(mb + t, nb) for t in range(1, nb)]
    spots = [lax.rem(spot + t, near) for t in range(1, near)]

    def remote(src, dst, send, recv, j, axis="ga"):
        return pltpu.make_async_remote_copy(
            src_ref=src, dst_ref=dst, send_sem=send, recv_sem=recv,
            device_id={axis: j}, device_id_type=MESH,
        )

    def stage_copy(i, slot):
        return pltpu.make_async_copy(
            beta.at[pl.ds(i * STAGE, STAGE)], stage.at[slot], stage_sem.at[slot]
        )

    def x_part(h, c, j):
        at = pl.ds(pl.multiple_of(j * slots + c * piece, 128), piece)
        return coeffs.at[:, h * part : (h + 1) * part, at]

    def o_part(h, c, j):
        at = pl.ds(pl.multiple_of(j * slots + c * piece, 128), piece)
        return out.at[:, h * part : (h + 1) * part, at]

    def own_x(h, c):
        return pltpu.make_async_copy(x_part(h, c, me), xbuf.at[h, c, :, me], own_sem.at[h, c])

    def x_copy(h, c, j, source):
        return remote(
            x_part(h, c, j), xbuf.at[h, c, :, source], xs.at[h, c, j], xr.at[h, c, source], j
        )

    def own_o(h, c):
        return pltpu.make_async_copy(obuf.at[h, c, :, me], o_part(h, c, me), oown.at[h, c])

    def o_copy(h, c, j, source):
        return remote(
            obuf.at[h, c, :, j], o_part(h, c, source), os_.at[h, c, j], or_.at[h, c, source], j
        )

    def u_copy(h, at, source):
        return remote(
            usend.at[h, :, at], urecv.at[h, source], us.at[h, at], ur.at[h, source],
            side * near + at,
        )

    def c_copy(h):
        return remote(csend.at[h], crecv.at[h], cs.at[h], cr.at[h], other)

    def d_copy(h, at, source):
        return remote(
            dsend.at[h], drecv.at[h, side * near + source], ds_.at[h, at],
            dr.at[h, side * near + source], side * near + at,
        )

    def b_copy(h, source):
        return remote(dsend.at[h], drecv.at[h, source], bs.at[h], dr.at[h, source], other)

    def f_copy(h, at, source):
        block = drecv.at[h, (1 - side) * near + source]
        return remote(
            block, block, fs.at[h, at], dr.at[h, (1 - side) * near + source], side * near + at
        )

    def e_copy(j, source):
        return remote(esend, erecv.at[source], es.at[j], er.at[source], j)

    def g_copy(j, source):
        return remote(gsend, grecv.at[source], gs.at[j], gr.at[source], j, "band")

    def send_x(h, c):
        for j in peers:
            x_copy(h, c, j, me).start()

    count = counts[0]

    def first_product(h, c):
        own_x(h, c).wait()
        for j in peers:
            x_copy(h, c, j, j).wait_recv()
        slot_ids = c * piece + lax.broadcasted_iota(jnp.int32, (2 * bands, piece), 1)
        block = xbuf[h, c].astype(jnp.float32).reshape(2 * bands, piece)
        xt[...] = jnp.where(slot_ids < count, block, 0.0).T.astype(jnp.bfloat16)

        def product(r, carry):
            at = pl.ds(pl.multiple_of(r * ROWS, ROWS), ROWS)
            term = jnp.dot(
                held[at, c * piece : (c + 1) * piece], xt[...], preferred_element_type=jnp.float32
            )
            if c > 0:
                term = term + acc[at, :]
            if c < PIECES - 1:
                acc[at, :] = term
            else:
                turned = term.T
                united = turned[:bands] + swap_pairs(turned[bands:], 1.0, -1.0)
                united = united.reshape(2, near, part, ROWS)
                usend[h, :, :, :, at] = united.astype(jnp.bfloat16)
            return carry

        lax.fori_loop(0, rows // ROWS, product, 0)

    def send_sums(h):
        for at in spots:
            u_copy(h, at, spot).start()

    def half_sums(h):
        same = usend[h, side, spot].astype(jnp.float32)
        away = usend[h, 1 - side, spot].astype(jnp.float32)
        for at in spots:
            u_copy(h, at, at).wait_recv()
            same = same + urecv[h, at, side].astype(jnp.float32)
            away = away + urecv[h, at, 1 - side].astype(jnp.float32)
        csend[h] = away.astype(jnp.bfloat16)
        c_copy(h).start()
        usum[h] = same

    def couple(h):
        c_copy(h).wait_recv()
        summed = usum[h] + crecv[h].astype(jnp.float32)
        most = (table.shape[0] + 1) // 2
        coupled = summed * table[most - 1 : most, :]
        for d in range(1 - most, most):
            if d:
                moved = pltpu.roll(summed, (-2 * d) % rows, 1)
                coupled = coupled + moved * table[most - 1 + d : most + d, :]
        low = coupled.astype(jnp.bfloat16)
        dsend[h] = low
        b_copy(h, me).start()
        for at in spots:
            d_copy(h, at, spot).start()
        drecv[h, me] = low
        bands_now = jnp.sum(summed * coupled, axis=1, keepdims=True) / beta.shape[0]
        lanes = lax.broadcasted_iota(jnp.int32, (part, own), 1)
        line = lax.broadcasted_iota(jnp.int32, (part, own), 0) + h * part
        row = jnp.sum(jnp.where(lanes == line, bands_now, 0.0), axis=0, keepdims=True)
        sofar = jnp.broadcast_to(jnp.sum(bands_now, axis=0, keepdims=True), esend.shape)
        if h == 0:
            energy[...] = row
            gsend[...] = sofar
        else:
            energy[...] = energy[...] + row
            esend[...] = gsend[...] + sofar
            for j in peers:
                e_copy(j, me).start()

    def pass_on(h):
        b_copy(h, other).wait_recv()
        for at in spots:
            f_copy(h, at, spot).start()

    def gather(h):
        for at in spots:
            d_copy(h, at, at).wait_recv()
            f_copy(h, at, at).wait_recv()
        real = drecv[h].astype(jnp.float32).reshape(bands, rows)
        dfull[:bands, :] = real.astype(jnp.bfloat16)
        dfull[bands:, :] = swap_pairs(real, -1.0, 1.0).astype(jnp.bfloat16)

    step = divisor(piece, 256, 128)

    def second_product(h, c):
        def apply(w, carry):
            lanes = pl.ds(pl.multiple_of(w * step, 128), step)
            slab = pl.ds(pl.multiple_of(c * piece + w * step, 128), step)
            result = jnp.dot(dfull[...], held[:, slab], preferred_element_type=jnp.float32)
            ids = c * piece + w * step + lax.broadcasted_iota(jnp.int32, result.shape, 1)
            result = jnp.where(ids < count, result, 0.0).reshape(2, n, part, step)
            obuf[h, c, :, :, :, lanes] = result.astype(jnp.bfloat16)
            return carry

        lax.fori_loop(0, piece // step, apply, 0)
        for j in peers:
            o_copy(h, c, j, me).start()
        own_o(h, c).start()

    stage_copy(0, 0).start()
    barrier = pltpu.get_barrier_semaphore()
    for j in peers:
        pl.semaphore_signal(barrier, inc=1, device_id={"ga": j}, device_id_type=MESH)
    for j in mates:
        pl.semaphore_signal(barrier, inc=1, device_id={"band": j}, device_id_type=MESH)
    pl.semaphore_wait(barrier, n - 1 + nb - 1)

    for c in range(PIECES):
        send_x(0, c)
    early = PIECES // 2
    for c in range(early):
        send_x(1, c)
    for h in range(HALVES):
        for c in range(PIECES):
            own_x(h, c).start()

    blocks = beta.shape[0] // STAGE
    width = divisor(slots, 512, 128)

    def lay(i, carry):
        slot = lax.rem(i, 2)

        @pl.when(i + 1 < blocks)
        def _():
            stage_copy(i + 1, 1 - slot).start()

        stage_copy(i, slot).wait()

        def cols(w, carry):
            at = pl.ds(pl.multiple_of(w * width, 128), width)
            held[pl.ds(pl.multiple_of(i * 2 * STAGE, 2 * STAGE), 2 * STAGE), at] = stage[
                slot, :, :, at
            ].reshape(2 * STAGE, width)
            return carry

        return lax.fori_loop(0, slots // width, cols, carry)

    lax.fori_loop(0, blocks, lay, 0)
    strips = diagonals(atoms[...], coupling[...])
    wide = rows // len(strips)
    for i, strip in enumerate(strips):
        table[:, i * wide : (i + 1) * wide] = strip

    for c in range(PIECES):
        first_product(0, c)
    send_sums(0)
    for c in range(early, PIECES - 1):
        send_x(1, c)
    first_product(1, 0)
    half_sums(0)
    send_x(1, PIECES - 1)
    first_product(1, 1)
    couple(0)
    for c in range(2, PIECES - 1):
        first_product(1, c)
    pass_on(0)
    first_product(1, PIECES - 1)
    send_sums(1)
    gather(0)
    second_product(0, 0)
    half_sums(1)
    second_product(0, 1)
    couple(1)
    for c in range(2, PIECES - 1):
        second_product(0, c)
    pass_on(1)
    second_product(0, PIECES - 1)
    gather(1)
    for c in range(PIECES):
        second_product(1, c)

    for j in peers:
        e_copy(j, me).wait_send()
    group = esend[...]
    for j in peers:
        e_copy(j, j).wait_recv()
        group = group + erecv[j]
    gsend[...] = group
    for j in mates:
        g_copy(j, mb).start()
    whole = group
    for j in mates:
        g_copy(j, j).wait_recv()
        whole = whole + grecv[j]
    total[...] = whole[:1, :1] / math.sqrt(n * nb * own)

    for j in mates:
        g_copy(j, mb).wait_send()
    for h in range(HALVES):
        for c in range(PIECES):
            for j in peers:
                x_copy(h, c, j, me).wait_send()
                o_copy(h, c, j, me).wait_send()
                o_copy(h, c, j, j).wait_recv()
            own_o(h, c).wait()
        for at in spots:
            u_copy(h, at, spot).wait_send()
            d_copy(h, at, spot).wait_send()
            f_copy(h, at, spot).wait_send()
        c_copy(h).wait_send()
        b_copy(h, me).wait_send()


def shards(n, nb, coeffs, projectors, block_coupling, atom_counts, wave_counts):
    own = coeffs.shape[1]
    count, _, slots = projectors.shape
    most = block_coupling.shape[1]
    rows = 2 * count
    part = own // HALVES
    bands = n * part
    near = n // 2
    piece = slots // PIECES
    low, full = jnp.bfloat16, jnp.float32
    dma = pltpu.SemaphoreType.DMA
    out, energy, total = pl.pallas_call(
        functools.partial(kernel, n, nb),
        out_shape=(
            jax.ShapeDtypeStruct(coeffs.shape, low),
            jax.ShapeDtypeStruct((1, own), full),
            jax.ShapeDtypeStruct((1, 1), full),
        ),
        in_specs=[
            pl.BlockSpec(memory_space=pltpu.SMEM),
            pl.BlockSpec(memory_space=pltpu.HBM),
            pl.BlockSpec(memory_space=pltpu.HBM),
            pl.BlockSpec(memory_space=pltpu.VMEM),
            pl.BlockSpec(memory_space=pltpu.VMEM),
        ],
        out_specs=(
            pl.BlockSpec(memory_space=pl.ANY),
            pl.BlockSpec(memory_space=pltpu.VMEM),
            pl.BlockSpec(memory_space=pltpu.VMEM),
        ),
        scratch_shapes=[
            pltpu.VMEM((2, STAGE, 2, slots), low),
            pltpu.VMEM((rows, slots), low),
            pltpu.VMEM((HALVES, PIECES, 2, n, part, piece), low),
            pltpu.VMEM((piece, 2 * bands), low),
            pltpu.VMEM((rows, 2 * bands), full),
            pltpu.VMEM((2 * most - 1, rows), full),
            pltpu.VMEM((HALVES, 2, near, part, rows), low),
            pltpu.VMEM((HALVES, near, 2, part, rows), low),
            pltpu.VMEM((HALVES, part, rows), full),
            pltpu.VMEM((HALVES, part, rows), low),
            pltpu.VMEM((HALVES, part, rows), low),
            pltpu.VMEM((HALVES, part, rows), low),
            pltpu.VMEM((HALVES, n, part, rows), low),
            pltpu.VMEM((2 * bands, rows), low),
            pltpu.VMEM((HALVES, PIECES, 2, n, part, piece), low),
            pltpu.VMEM((8, 128), full),
            pltpu.VMEM((n, 8, 128), full),
            pltpu.VMEM((8, 128), full),
            pltpu.VMEM((nb, 8, 128), full),
            dma((2,)),
            dma((HALVES, PIECES)),
            dma((HALVES, PIECES, n)),
            dma((HALVES, PIECES, n)),
            dma((HALVES, near)),
            dma((HALVES, near)),
            dma((HALVES,)),
            dma((HALVES,)),
            dma((HALVES, near)),
            dma((HALVES, near)),
            dma((HALVES,)),
            dma((HALVES, n)),
            dma((HALVES, PIECES, n)),
            dma((HALVES, PIECES, n)),
            dma((n,)),
            dma((n,)),
            dma((nb,)),
            dma((nb,)),
            dma((HALVES, PIECES)),
        ],
        compiler_params=pltpu.CompilerParams(
            collective_id=0, has_side_effects=True, vmem_limit_bytes=50 * 2**20
        ),
        cost_estimate=pl.CostEstimate(
            flops=8 * rows * slots * n * own, bytes_accessed=2 * rows * slots, transcendentals=0
        ),
    )(wave_counts, coeffs, projectors, block_coupling.T, atom_counts.reshape(1, -1))
    return (out, energy.reshape(own), total.reshape(()))


def solution(mesh):
    placed = (P(None, ("ga", "band"), None), P(None, None, "ga"), P(), P(), P("ga"))
    return jax.shard_map(
        functools.partial(shards, mesh.shape["ga"], mesh.shape["band"]),
        mesh=mesh,
        in_specs=placed,
        out_specs=(P(None, ("ga", "band"), None), P(("ga", "band")), P()),
        check_vma=False,
    )
```
